32 devices in a mesh: groups: 2 (over y), expert: 4 (over x, core), etp: 4 (over z).
Axes of the slice: x: 2, y: 2, z: 4, core: 2. Of those that a mesh axis runs over, the one named last changes fastest.
Arguments:
- tokens: bfloat16 [1024, 4096], P(('groups', 'expert'), 'etp'), parts along dimension 0, may hold values from -6 to 6
- route_ids: int32 [1024, 2], P(('groups', 'expert')), parts along dimension 0, may hold values from 0 to 3, all different within a row; in each aligned block of 128 rows (0 to 127, 128 to 255, ...) at most 96 rows name the same one
- gate_weights: float32 [1024, 2], P(('groups', 'expert')), parts along dimension 0, may hold values from 0.2 to 1
- w_gate: bfloat16 [4, 4096, 14336], P('expert', None, 'etp'), may hold values from -0.09375 to 0.09375
- w_up: bfloat16 [4, 4096, 14336], P('expert', None, 'etp'), may hold values from -0.09375 to 0.09375
- w_down: bfloat16 [4, 14336, 4096], P('expert', 'etp'), may hold values from -0.0625 to 0.0625
Outputs:
- mixed: bfloat16 [1024, 4096], P(('groups', 'expert'), 'etp'), parts along dimension 0
The draws below stay inside these ranges and needn't reach their ends.
There are 2 independent parts, one for each index of `groups`. The reference program is written for one: setup_inputs(seed, part) draws one part's arguments, and reference() takes and returns one part's arrays. A program takes and returns all parts, laid end to end along the dimension named above; an argument that names none is the same for every part. Nothing has to cross between parts.
Inputs may be any that keep to these rules, and one draw needn't show every extreme that they name: `route_ids`: each row names two different experts. In the rows of one index of expert (128 aligned rows), no expert is named by more than 96 rows, a bound that some block reaches.
All inputs are finite; a program needn't handle non-finite values.
Results may differ from the reference program's by a relative error of at most 0.024.
Values may be sent and summed in bfloat16 or wider, within the bound.
A program may use at most 192 MiB of HBM per device.

```python
import math
import jax
import jax.numpy as jnp
import numpy as np
from jax import lax

D = 4096
FF = 14336
TOK_DEV = 128
CAP = 96
EXPERTS = 4
TOKENS = 512
N_EXPERT = 4
N_ETP = 4


def spiked(drawn, key, source, target, parts, factor):
    owner, partner = [(jnp.arange(drawn.shape[dim]) // (drawn.shape[dim] // parts)).reshape([-1 if axis == dim else 1 for axis in range(drawn.ndim)]) for dim in (source, target)]
    chosen = jax.random.permutation(key, parts)[partner]
    strong = (owner == chosen) | (owner == (partner + parts // 2) % parts)
    return jnp.where(strong, factor * drawn, drawn)


def shard_levels(key, dims, pieces, smallest, largest):
    level = 1.0
    for dim, blocks in pieces:
        heights = jax.random.uniform(jax.random.fold_in(jax.random.fold_in(key, 6), dim), (blocks,), jnp.float32, smallest / len(pieces), largest / len(pieces))
        level = level * jnp.repeat(jnp.exp(heights), dims[dim] // blocks).reshape((-1,) + (1,) * (len(dims) - 1 - dim))
    return level


def shared_out(rng, own, number, rows, amount, top, limit, skew):
    ranking = jax.random.permutation(rng, amount)
    packed, ordinary = shares(amount, rows * top, limit, skew, True), shares(amount, rows * top, limit, skew, False)
    places = jnp.arange(amount)

    def named(sizes, offset_by):
        used = int((sizes > 0).sum())
        fixed = max(1, used // 4)
        passed = fixed + (places - fixed + offset_by * (used - fixed)) % max(1, amount - fixed)
        return jnp.zeros((amount,), jnp.int32).at[ranking[jnp.where(places < fixed, places, passed)]].set(jnp.asarray(sizes, jnp.int32))

    sizes = jnp.where(number % 4 == 0, named(packed, number // 4), named(ordinary, number - number // 4 - 1))
    mixed = jax.random.permutation(jax.random.fold_in(own, 3), amount)
    source_of, taker = mixed[0:amount // 2 * 2:2], mixed[1:amount // 2 * 2:2]
    room = jnp.minimum(sizes[source_of] - 1, limit - sizes[taker]) // 2
    room = jnp.where((source_of == ranking[0]) | (taker == ranking[0]) | (sizes[taker] == 0), 0, jnp.maximum(room, 0))
    passed = jax.random.randint(jax.random.fold_in(own, 4), (amount // 2,), 0, 1 << 20) % (room + 1)
    sizes = sizes.at[source_of].add(-passed).at[taker].add(passed)
    members = jnp.searchsorted(jnp.cumsum(sizes), jnp.arange(rows * top), side="right").astype(jnp.int32)
    table = members.reshape(top, rows).T
    table = table[jax.random.permutation(jax.random.fold_in(own, 1), rows)]
    offset_by = jax.random.randint(jax.random.fold_in(own, 2), (rows, 1), 0, top)
    return jnp.take_along_axis(table, (jnp.arange(top)[None, :] + offset_by) % top, axis=1)


def shares(number_of, total, reach, skew, full):
    portions = [(1 << 20) // math.isqrt(rank ** skew) + 1 for rank in range(1, number_of + 1)]
    largest = reach if full else min(reach, max(-(-total // number_of), total * portions[0] // sum(portions)))
    least = 1 if total - largest >= number_of - 1 else 0
    counts, spare = [largest] + [least] * (number_of - 1), total - largest - least * (number_of - 1)
    while spare > 0:
        movable = [i for i in range(1, number_of) if counts[i] < largest] or [i for i in range(1, number_of) if counts[i] < reach]
        pool, budget = sum([portions[i] for i in movable]), spare
        for i in movable:
            more = min(reach - counts[i], max(1, budget * portions[i] // pool), spare)
            counts[i] = counts[i] + more
            spare = spare - more
    return np.array(counts)


def noise(rng, dims, spread, limit, cuts=(), held_as=jnp.bfloat16):
    drawn = jax.random.normal(rng, dims, jnp.float32) * spread
    if len(cuts) > 0:
        drawn = shard_levels(rng, dims, cuts, -0.22, 0.18) * drawn
    return jnp.clip(drawn, min=-limit, max=limit).astype(held_as)


def bell_draw_with(key, extent, width, limit, shards, heavy, kind=jnp.bfloat16):
    result = width * jax.random.normal(key, extent, jnp.float32)
    if shards:
        result = result * shard_levels(key, extent, shards, -0.22, 0.18)
    return jnp.clip(spiked(result, jax.random.fold_in(key, 3), *heavy), -limit, limit).astype(kind)


def setup_inputs(seed: int = 0, part: int = 0) -> dict:
    streams_of = jax.random.split(jax.random.key(seed), 7)
    part_splits = jax.random.split(jax.random.fold_in(streams_of[6], part), 7)
    tokens = noise(part_splits[0], (TOKENS, D), 1.0, 6.0, ((0, 4), (1, 4)))
    route_ids_keys = jax.random.split(jax.random.fold_in(part_splits[1], 1), TOKENS // TOK_DEV)
    route_ids_turns = jax.random.permutation(jax.random.fold_in(part_splits[1], 3), TOKENS // TOK_DEV)
    route_ids = jax.vmap(lambda own, number: shared_out(jax.random.fold_in(part_splits[1], 2), own, number, TOK_DEV, EXPERTS, 2, CAP, 1))(route_ids_keys, route_ids_turns).reshape((TOKENS, 2))
    gate_weights = jnp.clip(0.2 + 0.8 * jax.random.uniform(part_splits[2], (TOKENS, 2), jnp.float32) ** shard_levels(part_splits[2], (TOKENS, 2), ((0, 4),), -0.2, 0.2), 0.2, 1.0)
    w_gate = noise(streams_of[3], (EXPERTS, D, FF), D ** -0.5, 0.09375, ((0, 4), (2, 4)))
    w_up = noise(streams_of[4], (EXPERTS, D, FF), D ** -0.5, 0.09375, ((0, 4), (2, 4)))
    w_down = bell_draw_with(streams_of[5], (EXPERTS, FF, D), FF ** -0.5, 0.0625, ((0, 4), (1, 4)), (1, 2, 4, 2.0))
    return {"tokens": tokens, "route_ids": route_ids, "gate_weights": gate_weights, "w_gate": w_gate, "w_up": w_up, "w_down": w_down}


def down_sum(hidden_wide, down_wide):
    group = FF // N_ETP
    rows = hidden_wide.shape[0]

    def add_group(index, total):
        start = (index * group).astype(jnp.int32)
        hidden_part = lax.dynamic_slice_in_dim(hidden_wide, start, group, 1)
        down_part = lax.dynamic_slice_in_dim(down_wide, start, group, 0)
        partial_value = jnp.dot(hidden_part, down_part, precision=lax.Precision.HIGHEST).astype(jnp.bfloat16)
        return total + partial_value.astype(jnp.float32)

    return lax.fori_loop(0, N_ETP, add_group, jnp.zeros((rows, D), jnp.float32))


def reference(tokens, route_ids, gate_weights, w_gate, w_up, w_down):
    slot_total = N_EXPERT * CAP
    summed = jnp.zeros((TOKENS, D), jnp.float32)
    token_block = (jnp.arange(TOKENS, dtype=jnp.int32) // TOK_DEV).astype(jnp.int32)
    for expert_number in range(EXPERTS):
        hit_mask = route_ids == expert_number
        routed = jnp.any(hit_mask, axis=1).astype(jnp.int32)
        weighting = jnp.sum(jnp.where(hit_mask, gate_weights, 0.0), axis=1)
        slot_index = (jnp.cumsum(routed.reshape(N_EXPERT, TOK_DEV), axis=1) - 1).reshape(TOKENS).astype(jnp.int32)
        target_row = jnp.where(routed == 1, token_block * CAP + slot_index, slot_total).astype(jnp.int32)
        buffer = jnp.zeros((slot_total, D), jnp.bfloat16).at[target_row].set(tokens, mode="drop")
        buffer_wide = buffer.astype(jnp.float32)
        gate_sum = jnp.dot(buffer_wide, w_gate[expert_number].astype(jnp.float32), precision=lax.Precision.HIGHEST)
        up_sum = jnp.dot(buffer_wide, w_up[expert_number].astype(jnp.float32), precision=lax.Precision.HIGHEST)
        hidden = (jax.nn.silu(gate_sum) * up_sum).astype(jnp.bfloat16)
        expert_out = down_sum(hidden.astype(jnp.float32), w_down[expert_number].astype(jnp.float32)).astype(jnp.bfloat16)
        picked = expert_out[jnp.minimum(target_row, slot_total - 1)]
        summed = summed + weighting[:, None] * picked.astype(jnp.float32)
    return summed.astype(jnp.bfloat16)
```

```python
import functools

import jax
import jax.numpy as jnp
from jax import lax
from jax.experimental import pallas as pl
from jax.experimental.pallas import tpu as pltpu
from jax.sharding import PartitionSpec as P

CAP = 96


def shards(tokens, route_ids, gate_weights, w_gate, w_up, w_down):
    cycle_size = lax.axis_size("expert")
    token_count, local_width = tokens.shape
    slot_total = cycle_size * CAP
    expert_iota = lax.broadcasted_iota(jnp.int32, (1, 1, cycle_size), 2)
    hit_mask = route_ids[:, :, None] == expert_iota
    routed = jnp.any(hit_mask, axis=1).astype(jnp.int32)
    weighting = jnp.sum(jnp.where(hit_mask, gate_weights[:, :, None], 0.0), axis=1)
    slot_index = jnp.cumsum(routed, axis=0) - 1
    expert_base = lax.broadcasted_iota(jnp.int32, (1, cycle_size), 1) * CAP
    target_slot = jnp.where(routed == 1, expert_base + slot_index, -1)
    slot_iota = lax.broadcasted_iota(jnp.int32, (1, 1, slot_total), 2)
    pick_table = target_slot[:, :, None] == slot_iota
    select_table = jnp.any(pick_table, axis=1).astype(jnp.bfloat16)
    combine_table = jnp.sum(jnp.where(pick_table, weighting[:, :, None], 0.0), axis=1)
    dispatched = jnp.dot(select_table.T, tokens, preferred_element_type=jnp.float32)
    dispatched = dispatched.astype(jnp.bfloat16).reshape(cycle_size, CAP, local_width)
    gate_local = w_gate[0]
    up_local = w_up[0]
    down_local = w_down[0]
    received = lax.all_to_all(dispatched, "expert", split_axis=0, concat_axis=0, tiled=True)
    columns_in = lax.all_gather(
        received.reshape(slot_total, local_width), "etp", axis=1, tiled=True
    )
    gate_sum = jnp.dot(columns_in, gate_local, preferred_element_type=jnp.float32)
    up_sum = jnp.dot(columns_in, up_local, preferred_element_type=jnp.float32)
    hidden = (jax.nn.silu(gate_sum) * up_sum).astype(jnp.bfloat16)
    partial_out = jnp.dot(hidden, down_local, preferred_element_type=jnp.float32).astype(
        jnp.bfloat16
    )
    finished = (
        lax.psum_scatter(partial_out, "etp", scatter_dimension=1, tiled=True)
        .astype(jnp.float32)
        .astype(jnp.bfloat16)
    )
    results = lax.all_to_all(
        finished.reshape(cycle_size, CAP, local_width),
        "expert",
        split_axis=0,
        concat_axis=0,
        tiled=True,
    )
    flat_results = results.reshape(slot_total, local_width).astype(jnp.float32)
    mixed = jnp.dot(combine_table, flat_results, precision=lax.Precision.HIGHEST)
    return mixed.astype(jnp.bfloat16)


FOUR = 4
RING_IN = 8
RING_OUT = 5
TILE_IN = 512
TILE_OUT = 256
PIECE = 512


def partner(me, step):
    low = (me % 2 + step % 2) % 2
    high = (me // 2 + step // 2) % 2
    return low + 2 * high


def layer_kernel(
    tok_ref, meta_ref, gate_hbm, up_hbm, down_hbm, out_ref,
    metas, toks, chosen, pick, comb, acc_gate, acc_up, hidden,
    ring_in, ring_out, kept, core_out, core_in, x_out, x_in, z_out, z_in,
    sem_in, sem_out, meta_s, meta_r, z_s, z_r, x_s, x_r, ca_s, ca_r, cb_s, cb_r,
    rc_s, rc_r, rx_s, rx_r, rz_s, rz_r,
):
    rows, width = tok_ref.shape
    inner = gate_hbm.shape[2]
    e = lax.axis_index("expert")
    z = lax.axis_index("etp")
    tiles_in = inner // TILE_IN
    steps_in = FOUR * tiles_in
    pieces = width // PIECE
    per_piece = PIECE // TILE_OUT
    steps_out = FOUR * width // TILE_OUT
    order_out = (2, 3, 1, 0)

    def fetch_in(t, slot):
        row = pl.multiple_of(partner(z, t // tiles_in) * width, width)
        col = pl.multiple_of((t % tiles_in) * TILE_IN, TILE_IN)
        return [
            pltpu.make_async_copy(
                hbm.at[0, pl.ds(row, width), pl.ds(col, TILE_IN)],
                ring_in.at[slot, k],
                sem_in.at[slot, k],
            )
            for k, hbm in enumerate((gate_hbm, up_hbm))
        ]

    def fetch_out(u, slot):
        per_chunk = width // TILE_OUT
        index = u // per_chunk
        step = (2 + index) % FOUR * (1 - index // 2) + (3 - index) * (index // 2)
        col = partner(z, step) * width + (u % per_chunk) * TILE_OUT
        return pltpu.make_async_copy(
            down_hbm.at[0, :, pl.ds(pl.multiple_of(col, TILE_OUT), TILE_OUT)],
            ring_out.at[slot],
            sem_out.at[slot],
        )

    def send(source, target, s_sem, r_sem, axis, step):
        me = e if axis == "expert" else z
        return pltpu.make_async_remote_copy(
            src_ref=source, dst_ref=target, send_sem=s_sem, recv_sem=r_sem,
            device_id={axis: partner(me, step)},
            device_id_type=pl.DeviceIdType.MESH,
        )

    for t in range(RING_IN):
        for copy in fetch_in(t, t):
            copy.start()

    barrier = pltpu.get_barrier_semaphore()
    for step in range(1, FOUR):
        for axis, me in (("expert", e), ("etp", z)):
            pl.semaphore_signal(
                barrier, inc=1, device_id={axis: partner(me, step)},
                device_id_type=pl.DeviceIdType.MESH,
            )
    pl.semaphore_wait(barrier, 2 * (FOUR - 1))

    def block(i, j):
        return tok_ref if i == 0 and j == 0 else toks.at[i, j]

    meta_copies = [
        send(meta_ref, metas.at[j], meta_s.at[j], meta_r.at[j], "expert", j)
        for j in range(1, FOUR)
    ]
    z_copies = [None] + [
        send(tok_ref, toks.at[i, 0], z_s.at[i], z_r.at[i], "etp", i)
        for i in range(1, FOUR)
    ]
    x_copies = [
        send(block(i, 0), toks.at[i, 2], x_s.at[i], x_r.at[i], "expert", 2)
        for i in range(FOUR)
    ]
    ca_copies = [
        send(block(i, 0), toks.at[i, 1], ca_s.at[i], ca_r.at[i], "expert", 1)
        for i in range(FOUR)
    ]
    cb_copies = [
        send(toks.at[i, 2], toks.at[i, 3], cb_s.at[i], cb_r.at[i], "expert", 1)
        for i in range(FOUR)
    ]
    for copy in meta_copies:
        copy.start()
    x_copies[0].start()
    for i in range(1, FOUR):
        z_copies[i].start()
    ca_copies[0].start()

    for copy in meta_copies:
        copy.wait_recv()
    mine = e.astype(jnp.float32)
    earlier = (
        lax.broadcasted_iota(jnp.int32, (rows, rows), 0)
        < lax.broadcasted_iota(jnp.int32, (rows, rows), 1)
    ).astype(jnp.bfloat16)
    slot_row = lax.broadcasted_iota(jnp.int32, (rows, rows), 0).astype(jnp.float32)
    for j in range(FOUR):
        meta = meta_ref[...] if j == 0 else metas[j]
        first = meta[0:1, :] == mine
        second = meta[1:2, :] == mine
        routed = jnp.where(first, 1.0, 0.0) + jnp.where(second, 1.0, 0.0)
        weight = jnp.where(first, meta[2:3, :], 0.0) + jnp.where(second, meta[3:4, :], 0.0)
        slot = jnp.dot(
            jnp.broadcast_to(routed, (16, rows)).astype(jnp.bfloat16), earlier,
            preferred_element_type=jnp.float32,
        )[0:1, :]
        slot = jnp.where(routed > 0.5, slot, -1.0)
        hit = slot_row == slot
        pick[j] = jnp.where(hit, 1.0, 0.0).astype(jnp.bfloat16)
        comb[j] = jnp.where(hit, weight, 0.0).T.astype(jnp.bfloat16)

    for i in range(FOUR):
        if i + 1 < FOUR:
            z_copies[i + 1].wait_recv()
            x_copies[i + 1].start()
            ca_copies[i + 1].start()
        x_copies[i].wait_recv()
        cb_copies[i].start()
        if i == FOUR - 1:
            for u in range(RING_OUT):
                fetch_out(u, u).start()
        ca_copies[i].wait_recv()
        cb_copies[i].wait_recv()
        for j in range(FOUR):
            chosen[pl.ds(j * CAP, CAP), :] = jnp.dot(
                pick[j, 0:CAP, :], block(i, j)[...], preferred_element_type=jnp.float32
            ).astype(jnp.bfloat16)

        def in_step(n, carry, i=i):
            t = i * tiles_in + n
            slot = lax.rem(t, RING_IN)
            for copy in fetch_in(t, slot):
                copy.wait()
            col = pl.ds(pl.multiple_of(n * TILE_IN, TILE_IN), TILE_IN)
            gate = jnp.dot(chosen[...], ring_in[slot, 0], preferred_element_type=jnp.float32)
            up = jnp.dot(chosen[...], ring_in[slot, 1], preferred_element_type=jnp.float32)
            if i > 0:
                gate = gate + acc_gate[:, col]
                up = up + acc_up[:, col]
            if i < FOUR - 1:
                acc_gate[:, col] = gate
                acc_up[:, col] = up
            else:
                hidden[:, col] = (gate / (1.0 + jnp.exp(-gate)) * up).astype(jnp.bfloat16)

            @pl.when(t + RING_IN < steps_in)
            def _():
                for copy in fetch_in(t + RING_IN, slot):
                    copy.start()

            return carry

        lax.fori_loop(0, tiles_in, in_step, 0)

    total = FOUR * pieces
    core_copies = [
        send(core_out.at[s], core_in.at[s], rc_s.at[s], rc_r.at[s], "expert", 1)
        for s in range(total)
    ]
    rx_copies = [
        send(x_out.at[s], x_in.at[s], rx_s.at[s], rx_r.at[s], "expert", 2)
        for s in range(total)
    ]
    rz_copies = [
        send(z_out.at[s], z_in.at[s], rz_s.at[s], rz_r.at[s], "etp", order_out[s // pieces])
        for s in range(total - pieces)
    ]

    def down_piece(s):
        def out_step(q, carry):
            u = s * per_piece + q
            slot = lax.rem(u, RING_OUT)
            fetch_out(u, slot).wait()
            part = jnp.dot(
                hidden[...], ring_out[slot], preferred_element_type=jnp.float32
            ).astype(jnp.bfloat16)
            col = pl.ds(pl.multiple_of(q * TILE_OUT, TILE_OUT), TILE_OUT)
            for j in range(FOUR):
                share = jnp.dot(
                    comb[j, :, 0:CAP], part[j * CAP:(j + 1) * CAP, :],
                    preferred_element_type=jnp.float32,
                )
                if j % 2 == 0:
                    kept[s, j // 2, :, col] = share
                else:
                    core_out[s, j // 2, :, col] = share.astype(jnp.bfloat16)

            @pl.when(u + RING_OUT < steps_out)
            def _():
                fetch_out(u + RING_OUT, slot).start()

            return carry

        lax.fori_loop(0, per_piece, out_step, 0)
        core_copies[s].start()

    def x_stage(s):
        core_copies[s].wait_recv()
        x_out[s] = (kept[s, 1] + core_in[s, 1].astype(jnp.float32)).astype(jnp.bfloat16)
        rx_copies[s].start()

    def z_stage(s):
        rx_copies[s].wait_recv()
        both = kept[s, 0] + core_in[s, 0].astype(jnp.float32) + x_in[s].astype(jnp.float32)
        if s < total - pieces:
            z_out[s] = both.astype(jnp.bfloat16)
            rz_copies[s].start()
        else:
            kept[s, 0] = both

    LAG = 4
    for s in range(total):
        down_piece(s)
        if s >= 1:
            x_stage(s - 1)
        if s >= LAG:
            z_stage(s - LAG)
    x_stage(total - 1)
    for s in range(total - LAG, total):
        z_stage(s)
    for h in range(pieces):
        value = kept[total - pieces + h, 0]
        for index in range(FOUR - 1):
            s = index * pieces + h
            rz_copies[s].wait_recv()
            value = value + z_in[s].astype(jnp.float32)
        out_ref[:, h * PIECE:(h + 1) * PIECE] = value.astype(jnp.bfloat16)
    for copy in (
        meta_copies + z_copies[1:] + x_copies + ca_copies + cb_copies
        + core_copies + rx_copies + rz_copies
    ):
        copy.wait_send()


def fused(tokens, route_ids, gate_weights, w_gate, w_up, w_down):
    rows, width = tokens.shape
    inner = w_gate.shape[2]
    slots = FOUR * CAP
    total = FOUR * width // PIECE
    meta = jnp.concatenate(
        [route_ids.T.astype(jnp.float32), gate_weights.T, jnp.zeros((4, rows), jnp.float32)], axis=0
    )
    bf, f32 = jnp.bfloat16, jnp.float32
    dma = pltpu.SemaphoreType.DMA
    vmem = pl.BlockSpec(memory_space=pltpu.VMEM)
    hbm = pl.BlockSpec(memory_space=pl.ANY)
    return pl.pallas_call(
        layer_kernel,
        out_shape=jax.ShapeDtypeStruct((rows, width), bf),
        in_specs=[vmem, vmem, hbm, hbm, hbm],
        out_specs=vmem,
        scratch_shapes=[
            pltpu.VMEM((FOUR, 8, rows), f32),
            pltpu.VMEM((FOUR, FOUR, rows, width), bf),
            pltpu.VMEM((slots, width), bf),
            pltpu.VMEM((FOUR, rows, rows), bf),
            pltpu.VMEM((FOUR, rows, rows), bf),
            pltpu.VMEM((slots, inner), f32),
            pltpu.VMEM((slots, inner), f32),
            pltpu.VMEM((slots, inner), bf),
            pltpu.VMEM((RING_IN, 2, width, TILE_IN), bf),
            pltpu.VMEM((RING_OUT, inner, TILE_OUT), bf),
            pltpu.VMEM((total, 2, rows, PIECE), f32),
            pltpu.VMEM((total, 2, rows, PIECE), bf),
            pltpu.VMEM((total, 2, rows, PIECE), bf),
            pltpu.VMEM((total, rows, PIECE), bf),
            pltpu.VMEM((total, rows, PIECE), bf),
            pltpu.VMEM((total, rows, PIECE), bf),
            pltpu.VMEM((total, rows, PIECE), bf),
            dma((RING_IN, 2)), dma((RING_OUT,)),
            dma((FOUR,)), dma((FOUR,)), dma((FOUR,)), dma((FOUR,)),
            dma((FOUR,)), dma((FOUR,)), dma((FOUR,)), dma((FOUR,)),
            dma((FOUR,)), dma((FOUR,)),
            dma((total,)), dma((total,)), dma((total,)), dma((total,)),
            dma((total,)), dma((total,)),
        ],
        compiler_params=pltpu.CompilerParams(
            collective_id=0, has_side_effects=True, vmem_limit_bytes=67043328
        ),
    )(tokens, meta, w_gate, w_up, w_down)


def pick_body(tokens, route_ids, gate_weights, w_gate, w_up, w_down):
    square = lax.axis_size("expert") == FOUR and lax.axis_size("etp") == FOUR
    whole = tokens.shape[1] % PIECE == 0 and w_gate.shape[2] % TILE_IN == 0
    lanes = tokens.shape[0] == 128 and w_gate.shape[2] // TILE_IN * FOUR >= RING_IN
    body = fused if square and whole and lanes else shards
    return body(tokens, route_ids, gate_weights, w_gate, w_up, w_down)


def solution(mesh):
    return jax.shard_map(
        pick_body,
        mesh=mesh,
        in_specs=(
            P(("groups", "expert"), "etp"),
            P(("groups", "expert"), None),
            P(("groups", "expert"), None),
            P("expert", None, "etp"),
            P("expert", None, "etp"),
            P("expert", "etp", None),
        ),
        out_specs=P(("groups", "expert"), "etp"),
        check_vma=False,
    )
```

```python
import functools

import functools

import jax
import jax.numpy as jnp
from jax import lax
from jax.experimental import pallas as pl
from jax.experimental.pallas import tpu as pltpu
from jax.sharding import PartitionSpec as P

CAP = 96


def shards(tokens, route_ids, gate_weights, w_gate, w_up, w_down):
    cycle_size = lax.axis_size("expert")
    token_count, local_width = tokens.shape
    slot_total = cycle_size * CAP
    expert_iota = lax.broadcasted_iota(jnp.int32, (1, 1, cycle_size), 2)
    hit_mask = route_ids[:, :, None] == expert_iota
    routed = jnp.any(hit_mask, axis=1).astype(jnp.int32)
    weighting = jnp.sum(jnp.where(hit_mask, gate_weights[:, :, None], 0.0), axis=1)
    slot_index = jnp.cumsum(routed, axis=0) - 1
    expert_base = lax.broadcasted_iota(jnp.int32, (1, cycle_size), 1) * CAP
    target_slot = jnp.where(routed == 1, expert_base + slot_index, -1)
    slot_iota = lax.broadcasted_iota(jnp.int32, (1, 1, slot_total), 2)
    pick_table = target_slot[:, :, None] == slot_iota
    select_table = jnp.any(pick_table, axis=1).astype(jnp.bfloat16)
    combine_table = jnp.sum(jnp.where(pick_table, weighting[:, :, None], 0.0), axis=1)
    dispatched = jnp.dot(select_table.T, tokens, preferred_element_type=jnp.float32)
    dispatched = dispatched.astype(jnp.bfloat16).reshape(cycle_size, CAP, local_width)
    gate_local = w_gate[0]
    up_local = w_up[0]
    down_local = w_down[0]
    received = lax.all_to_all(dispatched, "expert", split_axis=0, concat_axis=0, tiled=True)
    columns_in = lax.all_gather(
        received.reshape(slot_total, local_width), "etp", axis=1, tiled=True
    )
    gate_sum = jnp.dot(columns_in, gate_local, preferred_element_type=jnp.float32)
    up_sum = jnp.dot(columns_in, up_local, preferred_element_type=jnp.float32)
    hidden = (jax.nn.silu(gate_sum) * up_sum).astype(jnp.bfloat16)
    partial_out = jnp.dot(hidden, down_local, preferred_element_type=jnp.float32).astype(
        jnp.bfloat16
    )
    finished = (
        lax.psum_scatter(partial_out, "etp", scatter_dimension=1, tiled=True)
        .astype(jnp.float32)
        .astype(jnp.bfloat16)
    )
    results = lax.all_to_all(
        finished.reshape(cycle_size, CAP, local_width),
        "expert",
        split_axis=0,
        concat_axis=0,
        tiled=True,
    )
    flat_results = results.reshape(slot_total, local_width).astype(jnp.float32)
    mixed = jnp.dot(combine_table, flat_results, precision=lax.Precision.HIGHEST)
    return mixed.astype(jnp.bfloat16)


FOUR = 4
RING_IN = 5
RING_OUT = 5
TILE_IN = 896
TILE_OUT = 256
PIECE = 512


def partner(me, step):
    low = (me % 2 + step % 2) % 2
    high = (me // 2 + step // 2) % 2
    return low + 2 * high


def layer_kernel(
    tok_ref, meta_ref, gate_hbm, up_hbm, down_hbm, out_ref,
    metas, toks, chosen, pick, comb, acc_gate, acc_up, hidden,
    ring_in, ring_out, kept, core_out, core_in, x_out, x_in, z_out, z_in,
    sem_in, sem_out, meta_s, meta_r, z_s, z_r, x_s, x_r, ca_s, ca_r, cb_s, cb_r,
    rc_s, rc_r, rx_s, rx_r, rz_s, rz_r,
):
    rows, width = tok_ref.shape
    inner = gate_hbm.shape[2]
    e = lax.axis_index("expert")
    z = lax.axis_index("etp")
    tiles_in = inner // TILE_IN
    steps_in = FOUR * tiles_in
    pieces = width // PIECE
    per_piece = PIECE // TILE_OUT
    steps_out = FOUR * width // TILE_OUT
    order_out = (2, 3, 1, 0)

    def fetch_in(t, slot):
        row = pl.multiple_of(partner(z, t // tiles_in) * width, width)
        col = pl.multiple_of((t % tiles_in) * TILE_IN, TILE_IN)
        return [
            pltpu.make_async_copy(
                hbm.at[0, pl.ds(row, width), pl.ds(col, TILE_IN)],
                ring_in.at[slot, :, pl.ds(k * TILE_IN, TILE_IN)],
                sem_in.at[slot, k],
            )
            for k, hbm in enumerate((gate_hbm, up_hbm))
        ]

    def fetch_out(u, slot):
        per_chunk = width // TILE_OUT
        index = u // per_chunk
        step = (2 + index) % FOUR * (1 - index // 2) + (3 - index) * (index // 2)
        col = partner(z, step) * width + (u % per_chunk) * TILE_OUT
        return pltpu.make_async_copy(
            down_hbm.at[0, :, pl.ds(pl.multiple_of(col, TILE_OUT), TILE_OUT)],
            ring_out.at[slot],
            sem_out.at[slot],
        )

    def send(source, target, s_sem, r_sem, axis, step):
        me = e if axis == "expert" else z
        return pltpu.make_async_remote_copy(
            src_ref=source, dst_ref=target, send_sem=s_sem, recv_sem=r_sem,
            device_id={axis: partner(me, step)},
            device_id_type=pl.DeviceIdType.MESH,
        )

    for t in range(RING_IN):
        for copy in fetch_in(t, t):
            copy.start()

    barrier = pltpu.get_barrier_semaphore()
    for step in range(1, FOUR):
        for axis, me in (("expert", e), ("etp", z)):
            pl.semaphore_signal(
                barrier, inc=1, device_id={axis: partner(me, step)},
                device_id_type=pl.DeviceIdType.MESH,
            )
    pl.semaphore_wait(barrier, 2 * (FOUR - 1))

    def block(i, j):
        return tok_ref if i == 0 and j == 0 else toks.at[i, j]

    meta_copies = [
        send(meta_ref, metas.at[j], meta_s.at[j], meta_r.at[j], "expert", j)
        for j in range(1, FOUR)
    ]
    z_copies = [None] + [
        send(tok_ref, toks.at[i, 0], z_s.at[i], z_r.at[i], "etp", i)
        for i in range(1, FOUR)
    ]
    x_copies = [
        send(block(i, 0), toks.at[i, 2], x_s.at[i], x_r.at[i], "expert", 2)
        for i in range(FOUR)
    ]
    ca_copies = [
        send(block(i, 0), toks.at[i, 1], ca_s.at[i], ca_r.at[i], "expert", 1)
        for i in range(FOUR)
    ]
    cb_copies = [
        send(toks.at[i, 2], toks.at[i, 3], cb_s.at[i], cb_r.at[i], "expert", 1)
        for i in range(FOUR)
    ]
    for copy in meta_copies:
        copy.start()
    x_copies[0].start()
    for i in range(1, FOUR):
        z_copies[i].start()
    ca_copies[0].start()

    for copy in meta_copies:
        copy.wait_recv()
    mine = e.astype(jnp.float32)
    earlier = (
        lax.broadcasted_iota(jnp.int32, (rows, rows), 0)
        < lax.broadcasted_iota(jnp.int32, (rows, rows), 1)
    ).astype(jnp.bfloat16)
    slot_row = lax.broadcasted_iota(jnp.int32, (rows, rows), 0).astype(jnp.float32)
    for j in range(FOUR):
        meta = meta_ref[...] if j == 0 else metas[j]
        first = meta[0:1, :] == mine
        second = meta[1:2, :] == mine
        routed = jnp.where(first, 1.0, 0.0) + jnp.where(second, 1.0, 0.0)
        weight = jnp.where(first, meta[2:3, :], 0.0) + jnp.where(second, meta[3:4, :], 0.0)
        slot = jnp.dot(
            jnp.broadcast_to(routed, (16, rows)).astype(jnp.bfloat16), earlier,
            preferred_element_type=jnp.float32,
        )[0:1, :]
        slot = jnp.where(routed > 0.5, slot, -1.0)
        hit = slot_row == slot
        pick[j] = jnp.where(hit, 1.0, 0.0).astype(jnp.bfloat16)
        comb[j] = jnp.where(hit, weight, 0.0).T.astype(jnp.bfloat16)

    def pass_on(i):
        z_copies[i].wait_recv()
        x_copies[i].start()
        ca_copies[i].start()

    def pass_over(i):
        x_copies[i].wait_recv()
        cb_copies[i].start()

    pass_on(1)
    pass_over(0)
    for i in range(FOUR):
        if i == FOUR - 1:
            for u in range(RING_OUT):
                fetch_out(u, u).start()
        ca_copies[i].wait_recv()
        cb_copies[i].wait_recv()
        for j in range(FOUR):
            chosen[pl.ds(j * CAP, CAP), :] = jnp.dot(
                pick[j, 0:CAP, :], block(i, j)[...], preferred_element_type=jnp.float32
            ).astype(jnp.bfloat16)

        def in_step(n, carry, i=i):
            if i + 2 < FOUR:
                pl.when(n == tiles_in // 2)(functools.partial(pass_on, i + 2))
            if i + 1 < FOUR:
                pl.when(n == tiles_in - 1)(functools.partial(pass_over, i + 1))
            t = i * tiles_in + n
            slot = lax.rem(t, RING_IN)
            for copy in fetch_in(t, slot):
                copy.wait()
            col = pl.ds(pl.multiple_of(n * TILE_IN, TILE_IN), TILE_IN)
            both = jnp.dot(chosen[...], ring_in[slot], preferred_element_type=jnp.float32)
            gate, up = both[:, :TILE_IN], both[:, TILE_IN:]
            if i > 0:
                gate = gate + acc_gate[:, col]
                up = up + acc_up[:, col]
            if i < FOUR - 1:
                acc_gate[:, col] = gate
                acc_up[:, col] = up
            else:
                hidden[:, col] = (gate / (1.0 + jnp.exp(-gate)) * up).astype(jnp.bfloat16)

            @pl.when(t + RING_IN < steps_in)
            def _():
                for copy in fetch_in(t + RING_IN, slot):
                    copy.start()

            return carry

        lax.fori_loop(0, tiles_in, in_step, 0)

    total = FOUR * pieces
    core_copies = [
        send(core_out.at[s], core_in.at[s], rc_s.at[s], rc_r.at[s], "expert", 1)
        for s in range(total)
    ]
    rx_copies = [
        send(x_out.at[s], x_in.at[s], rx_s.at[s], rx_r.at[s], "expert", 2)
        for s in range(total)
    ]
    rz_copies = [
        send(z_out.at[s], z_in.at[s], rz_s.at[s], rz_r.at[s], "etp", order_out[s // pieces])
        for s in range(total - pieces)
    ]

    def x_stage(s):
        core_copies[s].wait_recv()
        x_out[s] = (kept[s, 1] + core_in[s, 1].astype(jnp.float32)).astype(jnp.bfloat16)
        rx_copies[s].start()

    def z_stage(s):
        rx_copies[s].wait_recv()
        both = kept[s, 0] + core_in[s, 0].astype(jnp.float32) + x_in[s].astype(jnp.float32)
        if s < total - pieces:
            z_out[s] = both.astype(jnp.bfloat16)
            rz_copies[s].start()
        else:
            kept[s, 0] = both

    def down_piece(s):
        def out_step(q, carry):
            if s >= 1:
                pl.when(q == 1)(functools.partial(x_stage, s - 1))
            u = s * per_piece + q
            slot = lax.rem(u, RING_OUT)
            fetch_out(u, slot).wait()
            part = jnp.dot(
                hidden[...], ring_out[slot], preferred_element_type=jnp.float32
            ).astype(jnp.bfloat16)
            col = pl.ds(pl.multiple_of(q * TILE_OUT, TILE_OUT), TILE_OUT)
            for j in range(FOUR):
                share = jnp.dot(
                    comb[j, :, 0:CAP], part[j * CAP:(j + 1) * CAP, :],
                    preferred_element_type=jnp.float32,
                )
                if j % 2 == 0:
                    kept[s, j // 2, :, col] = share
                else:
                    core_out[s, j // 2, :, col] = share.astype(jnp.bfloat16)

            @pl.when(u + RING_OUT < steps_out)
            def _():
                fetch_out(u + RING_OUT, slot).start()

            return carry

        lax.fori_loop(0, per_piece, out_step, 0)
        core_copies[s].start()

    LAG = 3
    for s in range(total):
        down_piece(s)
        if s >= LAG:
            z_stage(s - LAG)
    x_stage(total - 1)
    for s in range(total - LAG, total):
        z_stage(s)
    for h in range(pieces):
        value = kept[total - pieces + h, 0]
        for index in range(FOUR - 1):
            s = index * pieces + h
            rz_copies[s].wait_recv()
            value = value + z_in[s].astype(jnp.float32)
        out_ref[:, h * PIECE:(h + 1) * PIECE] = value.astype(jnp.bfloat16)
    for copy in (
        meta_copies + z_copies[1:] + x_copies + ca_copies + cb_copies
        + core_copies + rx_copies + rz_copies
    ):
        copy.wait_send()


def fused(tokens, route_ids, gate_weights, w_gate, w_up, w_down):
    rows, width = tokens.shape
    inner = w_gate.shape[2]
    slots = FOUR * CAP
    total = FOUR * width // PIECE
    meta = jnp.concatenate(
        [route_ids.T.astype(jnp.float32), gate_weights.T, jnp.zeros((4, rows), jnp.float32)], axis=0
    )
    bf, f32 = jnp.bfloat16, jnp.float32
    dma = pltpu.SemaphoreType.DMA
    vmem = pl.BlockSpec(memory_space=pltpu.VMEM)
    hbm = pl.BlockSpec(memory_space=pl.ANY)
    return pl.pallas_call(
        layer_kernel,
        out_shape=jax.ShapeDtypeStruct((rows, width), bf),
        in_specs=[vmem, vmem, hbm, hbm, hbm],
        out_specs=vmem,
        scratch_shapes=[
            pltpu.VMEM((FOUR, 8, rows), f32),
            pltpu.VMEM((FOUR, FOUR, rows, width), bf),
            pltpu.VMEM((slots, width), bf),
            pltpu.VMEM((FOUR, rows, rows), bf),
            pltpu.VMEM((FOUR, rows, rows), bf),
            pltpu.VMEM((slots, inner), f32),
            pltpu.VMEM((slots, inner), f32),
            pltpu.VMEM((slots, inner), bf),
            pltpu.VMEM((RING_IN, width, 2 * TILE_IN), bf),
            pltpu.VMEM((RING_OUT, inner, TILE_OUT), bf),
            pltpu.VMEM((total, 2, rows, PIECE), f32),
            pltpu.VMEM((total, 2, rows, PIECE), bf),
            pltpu.VMEM((total, 2, rows, PIECE), bf),
            pltpu.VMEM((total, rows, PIECE), bf),
            pltpu.VMEM((total, rows, PIECE), bf),
            pltpu.VMEM((total, rows, PIECE), bf),
            pltpu.VMEM((total, rows, PIECE), bf),
            dma((RING_IN, 2)), dma((RING_OUT,)),
            dma((FOUR,)), dma((FOUR,)), dma((FOUR,)), dma((FOUR,)),
            dma((FOUR,)), dma((FOUR,)), dma((FOUR,)), dma((FOUR,)),
            dma((FOUR,)), dma((FOUR,)),
            dma((total,)), dma((total,)), dma((total,)), dma((total,)),
            dma((total,)), dma((total,)),
        ],
        compiler_params=pltpu.CompilerParams(
            collective_id=0, has_side_effects=True, vmem_limit_bytes=67043328
        ),
    )(tokens, meta, w_gate, w_up, w_down)


def pick_body(tokens, route_ids, gate_weights, w_gate, w_up, w_down):
    square = lax.axis_size("expert") == FOUR and lax.axis_size("etp") == FOUR
    whole = tokens.shape[1] % PIECE == 0 and w_gate.shape[2] % TILE_IN == 0
    lanes = tokens.shape[0] == 128 and w_gate.shape[2] // TILE_IN * FOUR >= RING_IN
    body = fused if square and whole and lanes else shards
    return body(tokens, route_ids, gate_weights, w_gate, w_up, w_down)


def solution(mesh):
    return jax.shard_map(
        pick_body,
        mesh=mesh,
        in_specs=(
            P(("groups", "expert"), "etp"),
            P(("groups", "expert"), None),
            P(("groups", "expert"), None),
            P("expert", None, "etp"),
            P("expert", None, "etp"),
            P("expert", "etp", None),
        ),
        out_specs=P(("groups", "expert"), "etp"),
        check_vma=False,
    )
```
